32 devices in a mesh: chan: 16 (over z, y, core), tm: 2 (over x).
Axes of the slice: x: 2, y: 2, z: 4, core: 2. Of those that a mesh axis runs over, the one named last changes fastest.
Arguments:
- voltages: bfloat16 [2, 512, 256, 512], P(None, None, 'chan', 'tm'), may hold values from -6 to 6, as said below
- flag_mask: int32 [4, 256], P('tm', 'chan'), may hold values from 0 to 1, as said below
- flagged_prefix_counts: int32 [4, 256], P('tm', 'chan'), may hold values from 0 to 127
Outputs:
- visibilities: float32 [512, 2, 256, 256], P(('chan', 'tm'))
The draws below stay inside these ranges and needn't reach their ends.
Inputs may be any that keep to these rules, and one draw needn't show every extreme that they name: `voltages`: samples that keep drops count as zero; a program may move only the kept samples, in any compact form. `flag_mask`: 1 keeps the block of 128 samples of an antenna, 0 drops it; some antennas are dropped in every block. The first flagged_prefix_counts samples of a kept block are flagged; flags and counts may be packed several to a word wherever they are moved.
All inputs are finite; a program needn't handle non-finite values.
Results may differ from the reference program's by a relative error of at most 0.0003.
Values may be sent and summed in bfloat16 or wider, within the bound.
A program may use at most 128 MiB of HBM per device.

```python
import jax
import jax.numpy as jnp
from jax import lax

ANTENNA_COUNT = 256
CHANNEL_COUNT = 512
FLAG_BLOCK_WIDTH = 128
FLAG_BLOCK_COUNT = 4
SAMPLE_COUNT = 512


def draw_voltages(key, part):
    value_key = jax.random.fold_in(key, 31)
    zero_key = jax.random.fold_in(key, 29)
    full_shape = (2, CHANNEL_COUNT, ANTENNA_COUNT, SAMPLE_COUNT)
    normal_values = jax.random.normal(value_key, full_shape, jnp.float32)
    values_drawn = jnp.clip(normal_values, -6.0, 6.0)
    silent = jax.random.randint(zero_key, (ANTENNA_COUNT, SAMPLE_COUNT), 0, 10) == 0
    return jnp.where(silent[None, None], 0.0, values_drawn).astype(jnp.bfloat16)


def draw_flag_mask(key, part):
    base = jax.random.fold_in(key, 17)
    initial_key, middle_key, final_key = jax.random.split(base, 3)
    valid_samples = (jax.random.randint(initial_key, (FLAG_BLOCK_COUNT, ANTENNA_COUNT), 0, 4) > 0).astype(jnp.int32)
    flagged_rows = jax.random.randint(middle_key, (ANTENNA_COUNT,), 0, 32) == 0
    selected_mask = jax.random.randint(final_key, (), 0, ANTENNA_COUNT)
    flagged_rows = flagged_rows | (jnp.arange(ANTENNA_COUNT) == selected_mask)
    return jnp.where(flagged_rows[None, :], 0, valid_samples).astype(jnp.int32)


def set_ends(result, rng, least, high):
    spot = [jax.random.randint(jax.random.fold_in(rng, axis), (), 0, length) for axis, length in enumerate(result.shape)]
    longest = result.shape.index(max(result.shape))
    neighbour = spot[:longest] + [(spot[longest] + 1) % result.shape[longest]] + spot[longest + 1:]
    return result.at[tuple(spot)].set(least).at[tuple(neighbour)].set(high)


def setup_inputs(seed: int = 0) -> dict:
    seeds = jax.random.split(jax.random.key(seed), 4)
    return {
        "voltages": draw_voltages(jax.random.fold_in(seeds[3], 71), 0),
        "flag_mask": draw_flag_mask(jax.random.fold_in(seeds[3], 71), 0),
        "flagged_prefix_counts": set_ends(jax.random.randint(seeds[2], (FLAG_BLOCK_COUNT, ANTENNA_COUNT), 0, FLAG_BLOCK_WIDTH), jax.random.fold_in(seeds[2], 1), 0, FLAG_BLOCK_WIDTH - 1).astype(jnp.int32),
    }


def pair_samples(flag_mask, flagged_prefix_counts):
    def add_block(total, block):
        live = block[0].astype(jnp.float32)
        cover = (FLAG_BLOCK_WIDTH - jnp.maximum(block[1][:, None], block[1][None, :])).astype(jnp.float32)
        return total + live[:, None] * live[None, :] * cover, 0

    start = jnp.zeros((flag_mask.shape[1], flag_mask.shape[1]), jnp.float32)
    total, unused = lax.scan(add_block, start, (flag_mask, flagged_prefix_counts))
    return total


def reference(voltages, flag_mask, flagged_prefix_counts):
    offsets = jnp.arange(FLAG_BLOCK_WIDTH, dtype=jnp.int32)
    retain_mask = (flag_mask.T[:, :, None] == 1) & (offsets[None, None, :] >= flagged_prefix_counts.T[:, :, None])
    retain_mask = retain_mask.reshape(ANTENNA_COUNT, SAMPLE_COUNT)
    width = 8

    def single_block(start):
        slab = lax.dynamic_slice_in_dim(voltages, start, width, 1)
        slab = jnp.where(retain_mask[None, None], slab, jnp.zeros((), slab.dtype)).astype(jnp.float32)
        real_part, imag_part = slab[0], slab[1]
        hp = lax.Precision.HIGHEST
        rr = jnp.einsum("cit,cjt->cij", real_part, real_part, precision=hp)
        ii = jnp.einsum("cit,cjt->cij", imag_part, imag_part, precision=hp)
        ir = jnp.einsum("cit,cjt->cij", imag_part, real_part, precision=hp)
        ri = jnp.einsum("cit,cjt->cij", real_part, imag_part, precision=hp)
        return jnp.stack([rr + ii, ir - ri], axis=1)

    block_offsets = jnp.arange(0, CHANNEL_COUNT, width, dtype=jnp.int32)
    visibility_matrix = lax.map(single_block, block_offsets).reshape(CHANNEL_COUNT, 2, ANTENNA_COUNT, ANTENNA_COUNT)
    pairs = pair_samples(flag_mask, flagged_prefix_counts)
    return visibility_matrix / jnp.maximum(pairs, 1.0)[None, None]
```

```python
import functools

import jax
import jax.numpy as jnp
from jax import lax
from jax.experimental import pallas as pl
from jax.experimental.pallas import tpu as pltpu
from jax.sharding import PartitionSpec as P

FLAG_BLOCK_WIDTH = 128
LANES = 128
MESH = pl.DeviceIdType.MESH
NT = (((1,), (1,)), ((), ()))


def exchange_kernel(
    n_chan, n_tm, spans, volt_ref, mask_ref, count_ref, out_ref,
    held, masks, counts, square, cols, keep, inverse, send_sem, recv_sem, table_send, table_recv,
):
    n = n_chan * n_tm
    channels = held.shape[1]
    groups = range(len(spans))
    antennas, samples = volt_ref.shape[2], volt_ref.shape[3]
    total_antennas = n_chan * antennas
    local_blocks = samples // FLAG_BLOCK_WIDTH
    my_chan, my_tm = lax.axis_index("chan"), lax.axis_index("tm")
    me = my_chan * n_tm + my_tm

    def swing(m):
        return (m + 1) // 2 * (1 - 2 * lax.rem(m + 1, 2))

    def hop(k):
        return n // 2 + swing(k - 1)

    def place(k):
        other = lax.rem(me + hop(k), n)
        return other, (other // n_tm, lax.rem(other, n_tm))

    barrier = pltpu.get_barrier_semaphore()

    def greet(k, carry):
        pl.semaphore_signal(barrier, inc=1, device_id=place(k)[1], device_id_type=MESH)
        return carry

    lax.fori_loop(1, n, greet, 0)
    pl.semaphore_wait(barrier, n - 1)

    def landing(g):
        return held.at[
            :, pl.ds(*spans[g]), my_chan, :, pl.ds(pl.multiple_of(my_tm * samples, LANES), samples)
        ]

    def flag_copy(k, which):
        source, table = ((mask_ref, masks), (count_ref, counts))[which]
        return pltpu.make_async_remote_copy(
            src_ref=source, dst_ref=table.at[me], send_sem=table_send.at[which, k],
            recv_sem=table_recv.at[which], device_id=place(k)[1], device_id_type=MESH,
        )

    def volt_copy(g, k):
        other, where = place(k)
        return pltpu.make_async_remote_copy(
            src_ref=volt_ref.at[:, pl.ds(other * channels + spans[g][0], spans[g][1])],
            dst_ref=landing(g), send_sem=send_sem.at[g, k], recv_sem=recv_sem.at[g],
            device_id=where, device_id_type=MESH,
        )

    def each(body):
        def run(k, carry):
            body(k)
            return carry

        lax.fori_loop(1, n, run, 0)

    for which in range(2):
        each(lambda k, which=which: flag_copy(k, which).start())
    for g in groups:
        each(lambda k, g=g: volt_copy(g, k).start())
    pltpu.make_async_copy(mask_ref, masks.at[me], table_recv.at[0]).start()
    pltpu.make_async_copy(count_ref, counts.at[me], table_recv.at[1]).start()
    for g in groups:
        pltpu.make_async_copy(
            volt_ref.at[:, pl.ds(me * channels + spans[g][0], spans[g][1])], landing(g), recv_sem.at[g]
        ).start()

    pltpu.make_async_copy(masks, masks, table_recv.at[0]).wait()
    pltpu.make_async_copy(counts, counts, table_recv.at[1]).wait()
    limits = jnp.where(masks[...] == 1, counts[...], FLAG_BLOCK_WIDTH).astype(jnp.float32)
    square[...] = jnp.zeros_like(square)
    for b in range(local_blocks):
        square[b, :n, :antennas] = limits[:, b, :]
    turned = [square[b].T for b in range(local_blocks)]
    lane = lax.broadcasted_iota(jnp.int32, (total_antennas, LANES), 1).astype(jnp.float32)
    pairs = jnp.zeros((total_antennas, total_antennas), jnp.float32)
    for t in range(n_tm):
        for b in range(local_blocks):
            q = t * local_blocks + b
            for c in range(n_chan):
                source = c * n_tm + t
                cols[c * antennas:(c + 1) * antennas, :] = jnp.broadcast_to(
                    turned[b][:antennas, source:source + 1], (antennas, LANES)
                )
            column = cols[...]
            keep[:, q * LANES:(q + 1) * LANES] = jnp.where(lane >= column, 1.0, 0.0).astype(keep.dtype)
            pairs += FLAG_BLOCK_WIDTH - jnp.maximum(column[:, :1], column.T[:1, :])
    inverse[...] = 1.0 / jnp.maximum(pairs, 1.0)

    def correlate(c, carry):
        size = (total_antennas, keep.shape[1])
        real = held[0, c].reshape(size) * keep[...]
        imag = held[1, c].reshape(size) * keep[...]
        same = lax.dot_general(real, real, NT, preferred_element_type=jnp.float32)
        same += lax.dot_general(imag, imag, NT, preferred_element_type=jnp.float32)
        cross = lax.dot_general(imag, real, NT, preferred_element_type=jnp.float32)
        out_ref[c, 0] = same * inverse[...]
        out_ref[c, 1] = (cross - cross.T) * inverse[...]
        return carry

    for g in groups:
        part = held.at[:, pl.ds(*spans[g])]
        pltpu.make_async_copy(part, part, recv_sem.at[g]).wait()
        lax.fori_loop(spans[g][0], sum(spans[g]), correlate, 0)

    for which in range(2):
        each(lambda k, which=which: flag_copy(k, which).wait_send())
    for g in groups:
        each(lambda k, g=g: volt_copy(g, k).wait_send())


def shards(n_chan, n_tm, voltages, flag_mask, flagged_prefix_counts):
    parts, all_channels, antennas, samples = voltages.shape
    n = n_chan * n_tm
    channels = all_channels // n
    total_antennas, total_samples = antennas * n_chan, samples * n_tm
    last = max(1, channels // 8)
    cuts = [(channels - last) * g // 3 for g in range(4)] + [channels]
    spans = [(a, b - a) for a, b in zip(cuts, cuts[1:]) if b > a]
    groups, blocks = len(spans), flag_mask.shape[0]
    return pl.pallas_call(
        functools.partial(exchange_kernel, n_chan, n_tm, spans),
        out_shape=pltpu.VMEM((channels, 2, total_antennas, total_antennas), jnp.float32),
        in_specs=[pl.BlockSpec(memory_space=pl.ANY)] * 3,
        out_specs=pl.BlockSpec(memory_space=pltpu.VMEM),
        scratch_shapes=[
            pltpu.VMEM((parts, channels, n_chan, antennas, total_samples), voltages.dtype),
            pltpu.VMEM((n, blocks, antennas), jnp.int32),
            pltpu.VMEM((n, blocks, antennas), jnp.int32),
            pltpu.VMEM((blocks, n + -n % LANES, LANES), jnp.float32),
            pltpu.VMEM((total_antennas, LANES), jnp.float32),
            pltpu.VMEM((total_antennas, total_samples), voltages.dtype),
            pltpu.VMEM((total_antennas, total_antennas), jnp.float32),
            pltpu.SemaphoreType.DMA((groups, n)),
            pltpu.SemaphoreType.DMA((groups,)),
            pltpu.SemaphoreType.DMA((2, n)),
            pltpu.SemaphoreType.DMA((2,)),
        ],
        compiler_params=pltpu.CompilerParams(
            collective_id=0, has_side_effects=True, vmem_limit_bytes=48 * 1024 * 1024
        ),
    )(voltages, flag_mask, flagged_prefix_counts)


def solution(mesh):
    placed = (P(None, None, "chan", "tm"), P("tm", "chan"), P("tm", "chan"))
    return jax.shard_map(
        functools.partial(shards, mesh.shape["chan"], mesh.shape["tm"]),
        mesh=mesh,
        in_specs=placed,
        out_specs=P(("chan", "tm"), None, None, None),
        check_vma=False,
    )
```
